32 devices in a mesh: dp: 4 (over y, x), seq: 8 (over z, core).
Axes of the slice: x: 2, y: 2, z: 4, core: 2. Of those that a mesh axis runs over, the one named last changes fastest.
Arguments:
- queries: bfloat16 [4, 2048, 16, 128], P('dp', 'seq'), may hold values from -9 to 9
- keys: bfloat16 [4, 2048, 8, 128], P('dp', 'seq'), may hold values from -9 to 9
- values: bfloat16 [4, 2048, 8, 128], P('dp', 'seq'), may hold values from -6 to 6
- doc_lengths: int32 [4, 8], P('dp'), may hold values from 1 to 1536, 2048 in all within a row
Outputs:
- attended: bfloat16 [4, 2048, 16, 128], P('dp', 'seq')
- z_loss: float32 [], replicated
The draws below stay inside these ranges and needn't reach their ends.
Inputs may be any that keep to these rules, and one draw needn't show every extreme that they name: `doc_lengths`: each row's 8 lengths add up to 2048, and its longest document has exactly 1536 tokens.
All inputs are finite; a program needn't handle non-finite values.
Results may differ from the reference program's by a relative error of at most 0.012.
Values may be sent and summed in bfloat16 or wider, within the bound.
A program may use at most 64 MiB of HBM per device.

```python
import math
import jax
import jax.numpy as jnp
import numpy as np
from jax import lax

HQ = 16
KVH = 8
HD = 128
WINDOW = 1024
DOCS = 8
TOK_DEV = 256
BATCH = 4
SEQ_LEN = 2048


def paired_vectors(key):
    query_shape = (BATCH, SEQ_LEN, HQ, HD)
    key_shape = (BATCH, SEQ_LEN, KVH, HD)
    query_draw = 1.5 * jnp.clip(jax.random.normal(jax.random.fold_in(key, 21), query_shape, jnp.float32), -6.0, 6.0)
    key_draw = 1.5 * jnp.clip(jax.random.normal(jax.random.fold_in(key, 22), key_shape, jnp.float32), -6.0, 6.0)
    return (query_draw, key_draw)


def draw_queries(key, part):
    return paired_vectors(key)[0].astype(jnp.bfloat16)


def draw_keys(key, part):
    return paired_vectors(key)[1].astype(jnp.bfloat16)


def steps_of(rng, dims, split, smallest, largest):
    factor_of, own = 1.0, jax.random.fold_in(rng, 6)
    for position, blocks in split:
        heights = jnp.exp(jax.random.uniform(jax.random.fold_in(own, position), (blocks,), jnp.float32, smallest / len(split), largest / len(split)))
        factor_of = factor_of * jnp.repeat(heights, dims[position] // blocks).reshape([-1 if axis == position else 1 for axis in range(len(dims))])
    return factor_of


def split_up(count, total, reach, lean):
    portions = [(1 << 20) // math.isqrt(rank ** lean) + 1 for rank in range(2, count + 1)]
    spare, given = total - reach - (count - 1), [1] * (count - 1)
    while spare > 0:
        candidates = [i for i in range(count - 1) if given[i] < reach]
        whole, left = sum([portions[i] for i in candidates]), spare
        for i in candidates:
            addition = min(reach - given[i], max(1, left * portions[i] // whole), spare)
            given[i] = given[i] + addition
            spare = spare - addition
    return np.array([reach] + given)


def ragged_sizes(rng, count, total, most, lean):
    if count == 2:
        one = jax.random.randint(rng, (), max(1, total - most), min(most, total - 1) + 1)
        return jnp.stack([one, total - one])
    lengths = jnp.asarray(split_up(count, total, most, lean), jnp.int32)
    pairs = (count - 1) // 2
    source_of, taker = lengths[1:1 + 2 * pairs:2], lengths[2:2 + 2 * pairs:2]
    slack = jnp.minimum(source_of - 1, most - taker)
    moved = jax.random.randint(jax.random.fold_in(rng, 1), (pairs,), 0, 1 << 20) % (slack + 1)
    lengths = lengths.at[1:1 + 2 * pairs:2].set(source_of - moved).at[2:2 + 2 * pairs:2].set(taker + moved)
    return lengths[jax.random.permutation(jax.random.fold_in(rng, 2), count)]


def gaussian(stream_key, extent, scale, most, cuts=(), kind=jnp.bfloat16):
    entries = jax.random.normal(stream_key, extent, jnp.float32) * scale
    if len(cuts) > 0:
        entries = steps_of(stream_key, extent, cuts, -0.22, 0.18) * entries
    return jnp.clip(entries, min=-most, max=most).astype(kind)


def setup_inputs(seed: int = 0) -> dict:
    arg_keys = jax.random.split(jax.random.key(seed), 5)
    return {
        "queries": draw_queries(jax.random.fold_in(arg_keys[4], 71), 0),
        "keys": draw_keys(jax.random.fold_in(arg_keys[4], 71), 0),
        "values": gaussian(arg_keys[2], (BATCH, SEQ_LEN, KVH, HD), 1.0, 6.0, ((0, 4), (1, 8))),
        "doc_lengths": jax.vmap(lambda own: ragged_sizes(own, DOCS, SEQ_LEN, 3 * SEQ_LEN // 4, 2))(jax.random.split(arg_keys[3], BATCH)).reshape((BATCH, DOCS)).astype(jnp.int32),
    }


rope_base = 500000.0
score_scale = 1.0 / 12.0
masked = -1.0e30


def rotate(tensor, places):
    half = tensor.shape[-1] // 2
    frequency = rope_base ** (-2.0 * jnp.arange(half, dtype=jnp.float32) / tensor.shape[-1])
    angles = places.astype(jnp.float32)[..., None, None] * frequency
    cos_table = jnp.cos(angles)
    sin_table = jnp.sin(angles)
    widened = tensor.astype(jnp.float32)
    front_half = widened[..., :half]
    back_half = widened[..., half:]
    joined = jnp.concatenate([front_half * cos_table - back_half * sin_table, back_half * cos_table + front_half * sin_table], axis=-1)
    return joined.astype(jnp.bfloat16)


def reference(queries, keys, values, doc_lengths):
    doc_ends = jnp.cumsum(doc_lengths, axis=1)
    doc_starts = doc_ends - doc_lengths
    all_rows = jnp.arange(SEQ_LEN, dtype=jnp.int32)
    doc_of = jnp.sum((doc_ends[:, None, :] <= all_rows[None, :, None]).astype(jnp.int32), axis=2)
    chosen = doc_of[:, :, None] == jnp.arange(DOCS, dtype=jnp.int32)[None, None, :]
    start_of = jnp.sum(jnp.where(chosen, doc_starts[:, None, :], 0), axis=2)
    places = all_rows[None, :] - start_of
    block = 512 if SEQ_LEN % 512 == 0 else TOK_DEV
    group_size = HQ // KVH

    def one_seq(operands):
        seq_queries, seq_keys, seq_values, seq_docs, seq_places = operands
        query_rot = rotate(seq_queries, seq_places)
        key_rot = rotate(seq_keys, seq_places)
        key_padded = jnp.pad(key_rot, ((WINDOW, 0), (0, 0), (0, 0)))
        value_padded = jnp.pad(seq_values, ((WINDOW, 0), (0, 0), (0, 0)))
        docs_padded = jnp.pad(seq_docs, (WINDOW, 0), constant_values=-1)

        def one_block(begin):
            query_block = lax.dynamic_slice_in_dim(query_rot, begin, block, 0).astype(jnp.float32)
            query_block = query_block.reshape(block, KVH, group_size, HD)
            key_block = lax.dynamic_slice_in_dim(key_padded, begin, WINDOW + block, 0).astype(jnp.float32)
            value_block = lax.dynamic_slice_in_dim(value_padded, begin, WINDOW + block, 0).astype(jnp.float32)
            query_docs = lax.dynamic_slice_in_dim(seq_docs, begin, block, 0)
            key_docs = lax.dynamic_slice_in_dim(docs_padded, begin, WINDOW + block, 0)
            query_at = begin + jnp.arange(block, dtype=jnp.int32)
            key_at = begin - WINDOW + jnp.arange(WINDOW + block, dtype=jnp.int32)
            visible = (query_docs[:, None] == key_docs[None, :]) & (key_at[None, :] <= query_at[:, None]) & (query_at[:, None] - key_at[None, :] < WINDOW)
            scores = jnp.einsum("tkgd,ukd->kgtu", query_block, key_block) * score_scale
            scores = jnp.where(visible[None, None], scores, masked)
            peak = jnp.max(scores, axis=-1)
            weights = jnp.where(visible[None, None], jnp.exp(scores - peak[..., None]), 0.0)
            total = jnp.sum(weights, axis=-1)
            rounded = weights.astype(jnp.bfloat16).astype(jnp.float32)
            mixed = jnp.einsum("kgtu,ukd->tkgd", rounded, value_block)
            mixed = mixed / jnp.transpose(total, (2, 0, 1))[..., None]
            return mixed.reshape(block, HQ, HD).astype(jnp.bfloat16), peak + jnp.log(total)

        begins = jnp.arange(SEQ_LEN // block, dtype=jnp.int32) * block
        outputs, normalizers = lax.map(one_block, begins)
        return outputs.reshape(SEQ_LEN, HQ, HD), jnp.sum(normalizers * normalizers)

    attended, squares = lax.map(one_seq, (queries, keys, values, doc_of, places))
    return attended, jnp.sum(squares) / (BATCH * SEQ_LEN * HQ)
```

```python
import functools
import math

import jax
import jax.numpy as jnp
import numpy as np
from jax import lax
from jax.experimental import pallas as pl
from jax.experimental.pallas import tpu as pltpu
from jax.sharding import PartitionSpec as P

WINDOW = 1024
rope_base = 500000.0
score_scale = 1.0 / 12.0
masked = -1e30
MESH = pl.DeviceIdType.MESH
CHUNKS = 4


def tables(rows, reach, width):
    half = width // 2
    frequency = rope_base ** (-2.0 * np.arange(half) / width)
    at = np.arange(rows)[None, :] - rows * np.arange(reach + 1)[:, None]
    angles = at[..., None] * frequency
    cos = np.concatenate([np.cos(angles)] * 2, axis=-1)
    sin = np.concatenate([-np.sin(angles), np.sin(angles)], axis=-1)
    return np.stack([cos, sin], axis=1).astype(np.float32)


def body(
    n, n_dp, reach, lengths, q_hbm, k_hbm, v_hbm, tab, out, z_out,
    q_raw, raw, stage, q_rot, weights, peaks, totals, acc, low, bias, mine, parts_seq, mine2, parts_dp,
    load_sem, z_send, z_recv, d_send, d_recv, s_send, s_recv, p_send, p_recv,
):
    rows, heads, width = k_hbm.shape
    q_heads = q_hbm.shape[1]
    group = q_heads // heads
    hops = reach // 2
    piece = rows // CHUNKS
    me = lax.axis_index("seq")
    dp = lax.axis_index("dp")
    core = lax.rem(me, 2)
    chip = me // 2
    other = me + 1 - 2 * core
    above = me + 2
    has_above = above < n
    first = core == 0
    second = core == 1

    loads = [
        pltpu.make_async_copy(k_hbm, raw.at[0, 0], load_sem.at[0]),
        pltpu.make_async_copy(v_hbm, raw.at[1, 0], load_sem.at[1]),
        pltpu.make_async_copy(q_hbm, q_raw, load_sem.at[2]),
    ]
    for load in loads:
        load.start()

    barrier = pltpu.get_barrier_semaphore()

    def greet_seq(j, _):
        pl.semaphore_signal(barrier, inc=1, device_id={"seq": lax.rem(me + j, n)}, device_id_type=MESH)
        return 0

    def greet_dp(j, _):
        pl.semaphore_signal(barrier, inc=1, device_id={"dp": lax.rem(dp + j, n_dp)}, device_id_type=MESH)
        return 0

    lax.fori_loop(1, n, greet_seq, 0)
    lax.fori_loop(1, n_dp, greet_dp, 0)

    peaks[...] = jnp.full_like(peaks, masked)
    totals[...] = jnp.zeros_like(totals)
    acc[...] = jnp.zeros_like(acc)
    row_at = me * rows + lax.broadcasted_iota(jnp.int32, (rows, width), 0)
    start = jnp.zeros((rows, width), jnp.int32)
    end = jnp.int32(0)
    for i in range(lengths.shape[1]):
        end = end + lengths[0, i]
        start = jnp.where(end <= row_at, end, start)
    low[...] = jnp.maximum(start, row_at - (WINDOW - 1)) - me * rows

    for load in loads:
        load.wait()
    pl.semaphore_wait(barrier, (n - 1) + (n_dp - 1))

    def up(kind, hop, i):
        return pltpu.make_async_remote_copy(
            src_ref=raw.at[kind, 2 * hop, pl.ds(i * piece, piece)],
            dst_ref=raw.at[kind, 2 * hop + 2, pl.ds(i * piece, piece)],
            send_sem=z_send.at[kind, hop, i],
            recv_sem=z_recv.at[kind, hop, i],
            device_id={"seq": above},
            device_id_type=MESH,
        )

    def across(kind, hop, i):
        there = 2 * hop + 1 - 2 * core
        slot = hop - core
        return pltpu.make_async_remote_copy(
            src_ref=raw.at[kind, 2 * hop, pl.ds(i * piece, piece)],
            dst_ref=raw.at[kind, there, pl.ds(i * piece, piece)],
            send_sem=d_send.at[kind, slot, i],
            recv_sem=d_recv.at[kind, slot, i],
            device_id={"seq": other},
            device_id_type=MESH,
        )

    def each(low_i, high_i, do):
        def step(i, _):
            do(i)
            return 0

        lax.fori_loop(low_i, high_i, step, 0)

    def send_up(kind, hop, a, b):
        @pl.when(has_above)
        def _():
            each(a, b, lambda i: up(kind, hop, i).start())

    send_up(0, 0, 0, CHUNKS)
    send_up(1, 0, 0, 1)

    @pl.when(first)
    def _():
        for kind in range(2):
            each(0, CHUNKS, lambda i: across(kind, 0, i).start())

    def take(kind, hop, a, b):
        def one(i):
            up(kind, hop - 1, i).wait_recv()
            if hop < hops:
                @pl.when(has_above)
                def _():
                    up(kind, hop, i).start()

                across(kind, hop, i).start()
            else:
                @pl.when(second)
                def _():
                    across(kind, hop, i).start()

        each(a, b, one)

    def take_across(kind, slot, a, b):
        def one(i):
            pltpu.make_async_remote_copy(
                src_ref=raw.at[kind, 0, pl.ds(i * piece, piece)],
                dst_ref=raw.at[kind, 2 * slot + 1, pl.ds(i * piece, piece)],
                send_sem=d_send.at[kind, slot, i],
                recv_sem=d_recv.at[kind, slot, i],
                device_id={"seq": other},
                device_id_type=MESH,
            ).wait_recv()

        each(a, b, one)

    stage[...] = q_raw[...].astype(jnp.float32).reshape(rows * q_heads, width)
    scale = score_scale * math.log2(math.e)

    def turn_q(h, _):
        for g in range(group):
            x = stage[pl.ds(h * group + g, rows, stride=q_heads), :]
            turned = x * tab[0, 0] + pltpu.roll(x, width // 2, 1) * tab[0, 1]
            q_rot[h, g * rows : (g + 1) * rows, :] = (turned * scale).astype(jnp.bfloat16)
        return 0

    lax.fori_loop(0, heads, turn_q, 0)

    lane = lax.broadcasted_iota(jnp.int32, (rows, width), 1)

    def score(d):
        stage[0 : rows * heads, :] = raw[0, d].astype(jnp.float32).reshape(rows * heads, width)
        key_at = lax.broadcasted_iota(jnp.int32, (rows, rows), 1) - d * rows
        query_at = lax.broadcasted_iota(jnp.int32, (rows, rows), 0)
        seen = (key_at >= low[:, 0:1]) & (key_at <= query_at)
        bias[...] = jnp.where(seen, 0.0, masked)

        def head(h, _):
            x = stage[pl.ds(h, rows, stride=heads), :]
            k = (x * tab[d, 0] + pltpu.roll(x, width // 2, 1) * tab[d, 1]).astype(jnp.bfloat16)
            for g in range(group):
                part = slice(g * rows, (g + 1) * rows)
                s = lax.dot_general(
                    q_rot[h, part, :], k, (((1,), (1,)), ((), ())), preferred_element_type=jnp.float32
                )
                s = s + bias[...]
                m = jnp.max(s, axis=1, keepdims=True)
                p = jnp.exp2(s - m)
                t = jnp.sum(p, axis=1, keepdims=True)
                weights[d, h, part, :] = p.astype(jnp.bfloat16)
                peaks[h, part, :] = jnp.where(lane == d, m, peaks[h, part, :])
                totals[h, part, :] = jnp.where(lane == d, t, totals[h, part, :])
            return 0

        lax.fori_loop(0, heads, head, 0)

    def mix(d, a, b):
        count = b - a
        stage[0 : count * heads, :] = raw[1, d, a:b].astype(jnp.float32).reshape(count * heads, width)

        def head(h, _):
            v = stage[pl.ds(h, count, stride=heads), :].astype(jnp.bfloat16)
            o = jnp.dot(weights[d, h, :, a:b], v, preferred_element_type=jnp.float32)
            acc[h] = acc[h] + peaks[h, :, d : d + 1] * o
            return 0

        lax.fori_loop(0, heads, head, 0)

    score(0)

    @pl.when(second)
    def _():
        take_across(0, 0, 0, CHUNKS)
        score(1)

    @pl.when(chip >= 1)
    def _():
        take(0, 1, 0, CHUNKS)

    send_up(1, 0, 1, CHUNKS)

    @pl.when(chip >= 1)
    def _():
        score(2)
        take_across(0, core, 0, CHUNKS)
        score(1 + 2 * core)
        take(1, 1, 0, 1)

    @pl.when(chip >= 2)
    def _():
        take(0, 2, 0, CHUNKS)
        score(4)

        @pl.when(first)
        def _():
            take_across(0, 1, 0, CHUNKS)
            score(3)

    def settle(h, square):
        m = peaks[h]
        peak = jnp.max(m, axis=1, keepdims=True)
        a = jnp.exp2(m - peak)
        total = jnp.sum(a * totals[h], axis=1, keepdims=True)
        peaks[h] = a / total
        lse = peak * math.log(2.0) + jnp.log(total)
        return square + jnp.sum(lse * lse, axis=0, keepdims=True)

    square = lax.fori_loop(0, heads, settle, jnp.zeros((1, 1), jnp.float32))
    mine[...] = jnp.broadcast_to(square, mine.shape)
    parts_seq[me] = jnp.broadcast_to(square, mine.shape)

    mix(0, 0, rows)

    def tell_seq(j):
        return pltpu.make_async_remote_copy(
            src_ref=mine, dst_ref=parts_seq.at[me], send_sem=s_send.at[j], recv_sem=s_recv.at[j],
            device_id={"seq": lax.rem(me + j, n)}, device_id_type=MESH,
        )

    def heard_seq(j):
        return pltpu.make_async_remote_copy(
            src_ref=mine, dst_ref=parts_seq.at[lax.rem(me + n - j, n)], send_sem=s_send.at[j], recv_sem=s_recv.at[j],
            device_id={"seq": lax.rem(me + j, n)}, device_id_type=MESH,
        )

    def tell_dp(j):
        return pltpu.make_async_remote_copy(
            src_ref=mine2, dst_ref=parts_dp.at[dp], send_sem=p_send.at[j], recv_sem=p_recv.at[j],
            device_id={"dp": lax.rem(dp + j, n_dp)}, device_id_type=MESH,
        )

    def heard_dp(j):
        return pltpu.make_async_remote_copy(
            src_ref=mine2, dst_ref=parts_dp.at[lax.rem(dp + n_dp - j, n_dp)], send_sem=p_send.at[j], recv_sem=p_recv.at[j],
            device_id={"dp": lax.rem(dp + j, n_dp)}, device_id_type=MESH,
        )

    each(1, n, lambda j: tell_seq(j).start())

    @pl.when(second)
    def _():
        take_across(1, 0, 0, CHUNKS)
        mix(1, 0, rows)

    @pl.when(chip >= 1)
    def _():
        take(1, 1, 1, CHUNKS)
        mix(2, 0, rows)

        @pl.when(first)
        def _():
            take_across(1, 0, 0, CHUNKS)
            mix(1, 0, rows)

        @pl.when(second)
        def _():
            take_across(1, 1, 0, CHUNKS)
            mix(3, 0, rows)

    each(1, n, lambda j: heard_seq(j).wait_recv())
    column = jnp.sum(parts_seq[...], axis=0)
    mine2[...] = column
    parts_dp[dp] = column

    middle = rows // 2

    @pl.when(chip >= 2)
    def _():
        take(1, 2, 0, CHUNKS // 2)
        mix(4, 0, middle)

        @pl.when(first)
        def _():
            take_across(1, 1, 0, CHUNKS // 2)
            mix(3, 0, middle)

    each(1, n_dp, lambda j: tell_dp(j).start())
    each(1, n_dp, lambda j: heard_dp(j).wait_recv())
    z_out[0, 0] = jnp.sum(jnp.sum(parts_dp[...], axis=0)[0:1, 0:1]) / (n_dp * n * rows * q_heads)

    @pl.when(chip >= 2)
    def _():
        take(1, 2, CHUNKS // 2, CHUNKS)
        mix(4, middle, rows)

        @pl.when(first)
        def _():
            take_across(1, 1, CHUNKS // 2, CHUNKS)
            mix(3, middle, rows)

    def give(h, _):
        for g in range(group):
            stage[pl.ds(h * group + g, rows, stride=q_heads), :] = acc[h, g * rows : (g + 1) * rows, :]
        return 0

    lax.fori_loop(0, heads, give, 0)
    out[...] = stage[...].reshape(rows, q_heads, width).astype(jnp.bfloat16)

    def sent_up(kind, hop):
        each(0, CHUNKS, lambda i: up(kind, hop, i).wait_send())

    def sent_across(kind, hop):
        each(0, CHUNKS, lambda i: across(kind, hop, i).wait_send())

    for kind in range(2):
        pl.when(has_above)(functools.partial(sent_up, kind, 0))
        pl.when(has_above & (chip >= 1))(functools.partial(sent_up, kind, 1))
        pl.when(first)(functools.partial(sent_across, kind, 0))
        pl.when(chip >= 1)(functools.partial(sent_across, kind, 1))
        pl.when(second & (chip >= 2))(functools.partial(sent_across, kind, 2))
    each(1, n, lambda j: tell_seq(j).wait_send())
    each(1, n_dp, lambda j: tell_dp(j).wait_send())


def shards(queries, keys, values, doc_lengths):
    _, rows, q_heads, width = queries.shape
    heads = keys.shape[2]
    group = q_heads // heads
    n = lax.axis_size("seq")
    n_dp = lax.axis_size("dp")
    reach = -(-(WINDOW - 1) // rows)
    assert n % 2 == 0 and reach == 4
    hops = reach // 2
    tab = jnp.asarray(tables(rows, reach, width))
    vmem = pl.BlockSpec(memory_space=pltpu.VMEM)
    smem = pl.BlockSpec(memory_space=pltpu.SMEM)
    anywhere = pl.BlockSpec(memory_space=pl.ANY)
    dma = pltpu.SemaphoreType.DMA
    out, z = pl.pallas_call(
        functools.partial(body, n, n_dp, reach),
        out_shape=(
            jax.ShapeDtypeStruct((rows, q_heads, width), jnp.bfloat16),
            jax.ShapeDtypeStruct((1, 1), jnp.float32),
        ),
        in_specs=[smem, anywhere, anywhere, anywhere, vmem],
        out_specs=(vmem, smem),
        scratch_shapes=[
            pltpu.VMEM((rows, q_heads, width), jnp.bfloat16),
            pltpu.VMEM((2, reach + 1, rows, heads, width), jnp.bfloat16),
            pltpu.VMEM((rows * q_heads, width), jnp.float32),
            pltpu.VMEM((heads, group * rows, width), jnp.bfloat16),
            pltpu.VMEM((reach + 1, heads, group * rows, rows), jnp.bfloat16),
            pltpu.VMEM((heads, group * rows, width), jnp.float32),
            pltpu.VMEM((heads, group * rows, width), jnp.float32),
            pltpu.VMEM((heads, group * rows, width), jnp.float32),
            pltpu.VMEM((rows, width), jnp.int32),
            pltpu.VMEM((rows, rows), jnp.float32),
            pltpu.VMEM((8, width), jnp.float32),
            pltpu.VMEM((n, 8, width), jnp.float32),
            pltpu.VMEM((8, width), jnp.float32),
            pltpu.VMEM((n_dp, 8, width), jnp.float32),
            dma((3,)),
            dma((2, hops, CHUNKS)),
            dma((2, hops, CHUNKS)),
            dma((2, hops, CHUNKS)),
            dma((2, hops, CHUNKS)),
            dma((n,)),
            dma((n,)),
            dma((n_dp,)),
            dma((n_dp,)),
        ],
        compiler_params=pltpu.CompilerParams(
            collective_id=0, has_side_effects=True, vmem_limit_bytes=60 * 1024 * 1024
        ),
        name="attend",
    )(doc_lengths, queries[0], keys[0], values[0], tab)
    return out[None], z[0, 0]


def solution(mesh):
    placed = (
        P("dp", "seq", None, None),
        P("dp", "seq", None, None),
        P("dp", "seq", None, None),
        P("dp", None),
    )
    return jax.shard_map(
        shards,
        mesh=mesh,
        in_specs=placed,
        out_specs=(P("dp", "seq", None, None), P()),
        check_vma=False,
    )
```

```python
import functools
import math

import jax
import jax.numpy as jnp
import numpy as np
from jax import lax
from jax.experimental import pallas as pl
from jax.experimental.pallas import tpu as pltpu
from jax.sharding import PartitionSpec as P

WINDOW = 1024
rope_base = 500000.0
score_scale = 1.0 / 12.0
masked = -1e30
MESH = pl.DeviceIdType.MESH
CHUNKS = 4
UNROLL = 2


def tables(rows, reach, width):
    half = width // 2
    frequency = rope_base ** (-2.0 * np.arange(half) / width)
    at = np.arange(rows)[None, :] - rows * np.arange(reach + 1)[:, None]
    angles = at[..., None] * frequency
    cos = np.concatenate([np.cos(angles)] * 2, axis=-1)
    sin = np.concatenate([-np.sin(angles), np.sin(angles)], axis=-1)
    return np.stack([cos, sin], axis=1).astype(np.float32)


def body(
    n, n_dp, reach, lengths, q_hbm, k_hbm, v_hbm, tab_hbm, out, z_out,
    tab, q_raw, raw, stage, spread, q_rot, weights, peaks, totals, acc, low, bias, mine, parts_seq, mine2, parts_dp,
    load_sem, z_send, z_recv, d_send, d_recv, s_send, s_recv, p_send, p_recv,
):
    rows, heads, width = k_hbm.shape
    q_heads = q_hbm.shape[1]
    group = q_heads // heads
    hops = reach // 2
    piece = rows // CHUNKS
    me = lax.axis_index("seq")
    dp = lax.axis_index("dp")
    core = lax.rem(me, 2)
    chip = me // 2
    other = me + 1 - 2 * core
    above = me + 2
    has_above = above < n
    first = core == 0
    second = core == 1

    loads = [
        pltpu.make_async_copy(k_hbm, raw.at[0, 0], load_sem.at[0]),
        pltpu.make_async_copy(v_hbm, raw.at[1, 0], load_sem.at[1]),
        pltpu.make_async_copy(q_hbm, q_raw, load_sem.at[2]),
        pltpu.make_async_copy(tab_hbm, tab, load_sem.at[3]),
    ]
    for load in loads:
        load.start()

    barrier = pltpu.get_barrier_semaphore()

    def greet_seq(j, _):
        pl.semaphore_signal(barrier, inc=1, device_id={"seq": lax.rem(me + j, n)}, device_id_type=MESH)
        return 0

    def greet_dp(j, _):
        pl.semaphore_signal(barrier, inc=1, device_id={"dp": lax.rem(dp + j, n_dp)}, device_id_type=MESH)
        return 0

    lax.fori_loop(1, n, greet_seq, 0)
    lax.fori_loop(1, n_dp, greet_dp, 0)

    peaks[...] = jnp.full_like(peaks, masked)
    totals[...] = jnp.zeros_like(totals)
    row_at = me * rows + lax.broadcasted_iota(jnp.int32, (rows, width), 0)
    start = jnp.zeros((rows, width), jnp.int32)
    end = jnp.int32(0)
    for i in range(lengths.shape[1]):
        end = end + lengths[0, i]
        start = jnp.where(end <= row_at, end, start)
    low[...] = jnp.maximum(start, row_at - (WINDOW - 1)) - me * rows

    loads[0].wait()
    loads[1].wait()
    pl.semaphore_wait(barrier, (n - 1) + (n_dp - 1))

    def up(kind, hop, i):
        return pltpu.make_async_remote_copy(
            src_ref=raw.at[kind, 2 * hop, pl.ds(i * piece, piece)],
            dst_ref=raw.at[kind, 2 * hop + 2, pl.ds(i * piece, piece)],
            send_sem=z_send.at[kind, hop, i],
            recv_sem=z_recv.at[kind, hop, i],
            device_id={"seq": above},
            device_id_type=MESH,
        )

    def across(kind, hop, i):
        there = 2 * hop + 1 - 2 * core
        slot = hop - core
        return pltpu.make_async_remote_copy(
            src_ref=raw.at[kind, 2 * hop, pl.ds(i * piece, piece)],
            dst_ref=raw.at[kind, there, pl.ds(i * piece, piece)],
            send_sem=d_send.at[kind, slot, i],
            recv_sem=d_recv.at[kind, slot, i],
            device_id={"seq": other},
            device_id_type=MESH,
        )

    def each(low_i, high_i, do):
        def step(i, _):
            do(i)
            return 0

        lax.fori_loop(low_i, high_i, step, 0)

    def send_up(kind, hop, a, b):
        @pl.when(has_above)
        def _():
            each(a, b, lambda i: up(kind, hop, i).start())

    send_up(0, 0, 0, CHUNKS)
    send_up(1, 0, 0, 1)

    @pl.when(first)
    def _():
        for kind in range(2):
            each(0, CHUNKS, lambda i: across(kind, 0, i).start())

    def take(kind, hop, a, b):
        def one(i):
            up(kind, hop - 1, i).wait_recv()
            if hop < hops:
                @pl.when(has_above)
                def _():
                    up(kind, hop, i).start()

                across(kind, hop, i).start()
            else:
                @pl.when(second)
                def _():
                    across(kind, hop, i).start()

        each(a, b, one)

    def take_across(kind, slot, a, b):
        def one(i):
            pltpu.make_async_remote_copy(
                src_ref=raw.at[kind, 0, pl.ds(i * piece, piece)],
                dst_ref=raw.at[kind, 2 * slot + 1, pl.ds(i * piece, piece)],
                send_sem=d_send.at[kind, slot, i],
                recv_sem=d_recv.at[kind, slot, i],
                device_id={"seq": other},
                device_id_type=MESH,
            ).wait_recv()

        each(a, b, one)

    loads[2].wait()
    loads[3].wait()

    stage[...] = q_raw[...].astype(jnp.float32).reshape(rows * q_heads, width)
    scale = score_scale * math.log2(math.e)

    def turn_q(h, _):
        for g in range(group):
            x = stage[pl.ds(h * group + g, rows, stride=q_heads), :]
            turned = x * tab[0, 0] + pltpu.roll(x, width // 2, 1) * tab[0, 1]
            q_rot[h, g * rows : (g + 1) * rows, :] = (turned * scale).astype(jnp.bfloat16)
        return 0

    lax.fori_loop(0, heads, turn_q, 0)

    lane = lax.broadcasted_iota(jnp.int32, (rows, width), 1)

    def score(d):
        stage[0 : rows * heads, :] = raw[0, d].astype(jnp.float32).reshape(rows * heads, width)
        key_at = lax.broadcasted_iota(jnp.int32, (rows, rows), 1) - d * rows
        query_at = lax.broadcasted_iota(jnp.int32, (rows, rows), 0)
        seen = (key_at >= low[:, 0:1]) & (key_at <= query_at)
        bias[...] = jnp.where(seen, 0.0, masked)

        def head(h, _):
            x = stage[pl.ds(h, rows, stride=heads), :]
            k = (x * tab[d, 0] + pltpu.roll(x, width // 2, 1) * tab[d, 1]).astype(jnp.bfloat16)
            for g in range(group):
                part = slice(g * rows, (g + 1) * rows)
                s = lax.dot_general(
                    q_rot[h, part, :], k, (((1,), (1,)), ((), ())), preferred_element_type=jnp.float32
                )
                s = s + bias[...]
                m = jnp.max(s, axis=1, keepdims=True)
                p = jnp.exp2(s - m)
                t = jnp.sum(p, axis=1, keepdims=True)
                weights[d, h, part, :] = p.astype(jnp.bfloat16)
                peaks[h, part, :] = jnp.where(lane == d, m, peaks[h, part, :])
                totals[h, part, :] = jnp.where(lane == d, t, totals[h, part, :])
            return 0

        lax.fori_loop(0, heads, head, 0)

    def mix(blocks, a, b, fresh=False, last=False):
        count = b - a
        for j, d in enumerate(blocks):
            stage[j * count * heads : (j + 1) * count * heads, :] = (
                raw[1, d, a:b].astype(jnp.float32).reshape(count * heads, width)
            )

        def head(h):
            o = None if fresh else acc[h]
            for j, d in enumerate(blocks):
                v = stage[pl.ds(j * count * heads + h, count, stride=heads), :].astype(jnp.bfloat16)
                more = jnp.dot(weights[d, h, :, a:b], v, preferred_element_type=jnp.float32)
                o = more if o is None else o + more
            if last:
                for g in range(group):
                    spread[pl.ds(h * group + g, rows, stride=q_heads), :] = o[g * rows : (g + 1) * rows]
            else:
                acc[h] = o

        def pair(i, _):
            for j in range(UNROLL):
                head(i * UNROLL + j)
            return 0

        lax.fori_loop(0, heads // UNROLL, pair, 0)

    score(0)

    @pl.when(second)
    def _():
        take_across(0, 0, 0, CHUNKS)
        score(1)

    @pl.when(chip >= 1)
    def _():
        take(0, 1, 0, CHUNKS)

    send_up(1, 0, 1, CHUNKS)

    @pl.when(chip >= 1)
    def _():
        score(2)
        take_across(0, core, 0, CHUNKS)
        score(1 + 2 * core)
        take(1, 1, 0, 1)

    @pl.when(chip >= 2)
    def _():
        take(0, 2, 0, CHUNKS)
        score(4)

        @pl.when(first)
        def _():
            take_across(0, 1, 0, CHUNKS)
            score(3)

    def settle(h, square):
        m = peaks[h]
        peak = jnp.max(m, axis=1, keepdims=True)
        a = jnp.exp2(m - peak)
        total = jnp.sum(a * totals[h], axis=1, keepdims=True)
        share = a / total
        for d in range(reach + 1):
            weights[d, h] = (weights[d, h].astype(jnp.float32) * share[:, d : d + 1]).astype(jnp.bfloat16)
        lse = peak * math.log(2.0) + jnp.log(total)
        return square + jnp.sum(lse * lse, axis=0, keepdims=True)

    square = lax.fori_loop(0, heads, settle, jnp.zeros((1, 1), jnp.float32))
    mine[...] = jnp.broadcast_to(square, mine.shape)
    parts_seq[me] = jnp.broadcast_to(square, mine.shape)

    @pl.when(chip >= 1)
    def _():
        take(1, 1, 1, 2)

    @pl.when(first)
    def _():
        mix((0,), 0, rows, fresh=True)

    @pl.when(second)
    def _():
        take_across(1, 0, 0, CHUNKS)
        mix((0, 1), 0, rows, fresh=True)

    def tell_seq(j):
        return pltpu.make_async_remote_copy(
            src_ref=mine, dst_ref=parts_seq.at[me], send_sem=s_send.at[j], recv_sem=s_recv.at[j],
            device_id={"seq": lax.rem(me + j, n)}, device_id_type=MESH,
        )

    def heard_seq(j):
        return pltpu.make_async_remote_copy(
            src_ref=mine, dst_ref=parts_seq.at[lax.rem(me + n - j, n)], send_sem=s_send.at[j], recv_sem=s_recv.at[j],
            device_id={"seq": lax.rem(me + j, n)}, device_id_type=MESH,
        )

    def tell_dp(j):
        return pltpu.make_async_remote_copy(
            src_ref=mine2, dst_ref=parts_dp.at[dp], send_sem=p_send.at[j], recv_sem=p_recv.at[j],
            device_id={"dp": lax.rem(dp + j, n_dp)}, device_id_type=MESH,
        )

    def heard_dp(j):
        return pltpu.make_async_remote_copy(
            src_ref=mine2, dst_ref=parts_dp.at[lax.rem(dp + n_dp - j, n_dp)], send_sem=p_send.at[j], recv_sem=p_recv.at[j],
            device_id={"dp": lax.rem(dp + j, n_dp)}, device_id_type=MESH,
        )

    each(1, n, lambda j: tell_seq(j).start())

    @pl.when(chip >= 1)
    def _():
        take(1, 1, 2, CHUNKS)
        take_across(1, core, 0, CHUNKS)
        mix((2, 1 + 2 * core), 0, rows)

    each(1, n, lambda j: heard_seq(j).wait_recv())
    column = jnp.sum(parts_seq[...], axis=0)
    mine2[...] = column
    parts_dp[dp] = column

    middle = rows // 2

    @pl.when(chip >= 2)
    def _():
        take(1, 2, 0, CHUNKS // 2)

        @pl.when(second)
        def _():
            mix((4,), 0, middle)

        @pl.when(first)
        def _():
            take_across(1, 1, 0, CHUNKS // 2)
            mix((4, 3), 0, middle)

    each(1, n_dp, lambda j: tell_dp(j).start())
    each(1, n_dp, lambda j: heard_dp(j).wait_recv())
    z_out[0, 0] = jnp.sum(jnp.sum(parts_dp[...], axis=0)[0:1, 0:1]) / (n_dp * n * rows * q_heads)

    @pl.when(chip >= 2)
    def _():
        take(1, 2, CHUNKS // 2, CHUNKS)

        @pl.when(second)
        def _():
            mix((4,), middle, rows, last=True)

        @pl.when(first)
        def _():
            take_across(1, 1, CHUNKS // 2, CHUNKS)
            mix((4, 3), middle, rows, last=True)

    def give(h, _):
        for g in range(group):
            spread[pl.ds(h * group + g, rows, stride=q_heads), :] = acc[h, g * rows : (g + 1) * rows, :]
        return 0

    @pl.when(chip < 2)
    def _():
        lax.fori_loop(0, heads, give, 0)

    out[...] = spread[...].reshape(rows, q_heads, width).astype(jnp.bfloat16)

    def sent_up(kind, hop):
        each(0, CHUNKS, lambda i: up(kind, hop, i).wait_send())

    def sent_across(kind, hop):
        each(0, CHUNKS, lambda i: across(kind, hop, i).wait_send())

    for kind in range(2):
        pl.when(has_above)(functools.partial(sent_up, kind, 0))
        pl.when(has_above & (chip >= 1))(functools.partial(sent_up, kind, 1))
        pl.when(first)(functools.partial(sent_across, kind, 0))
        pl.when(chip >= 1)(functools.partial(sent_across, kind, 1))
        pl.when(second & (chip >= 2))(functools.partial(sent_across, kind, 2))
    each(1, n, lambda j: tell_seq(j).wait_send())
    each(1, n_dp, lambda j: tell_dp(j).wait_send())


def shards(queries, keys, values, doc_lengths):
    _, rows, q_heads, width = queries.shape
    heads = keys.shape[2]
    group = q_heads // heads
    n = lax.axis_size("seq")
    n_dp = lax.axis_size("dp")
    reach = -(-(WINDOW - 1) // rows)
    assert n % 2 == 0 and reach == 4
    hops = reach // 2
    tab = jnp.asarray(tables(rows, reach, width))
    vmem = pl.BlockSpec(memory_space=pltpu.VMEM)
    smem = pl.BlockSpec(memory_space=pltpu.SMEM)
    anywhere = pl.BlockSpec(memory_space=pl.ANY)
    dma = pltpu.SemaphoreType.DMA
    out, z = pl.pallas_call(
        functools.partial(body, n, n_dp, reach),
        out_shape=(
            jax.ShapeDtypeStruct((rows, q_heads, width), jnp.bfloat16),
            jax.ShapeDtypeStruct((1, 1), jnp.float32),
        ),
        in_specs=[smem, anywhere, anywhere, anywhere, anywhere],
        out_specs=(vmem, smem),
        scratch_shapes=[
            pltpu.VMEM(tab.shape, jnp.float32),
            pltpu.VMEM((rows, q_heads, width), jnp.bfloat16),
            pltpu.VMEM((2, reach + 1, rows, heads, width), jnp.bfloat16),
            pltpu.VMEM((rows * q_heads, width), jnp.float32),
            pltpu.VMEM((rows * q_heads, width), jnp.float32),
            pltpu.VMEM((heads, group * rows, width), jnp.bfloat16),
            pltpu.VMEM((reach + 1, heads, group * rows, rows), jnp.bfloat16),
            pltpu.VMEM((heads, group * rows, width), jnp.float32),
            pltpu.VMEM((heads, group * rows, width), jnp.float32),
            pltpu.VMEM((heads, group * rows, width), jnp.float32),
            pltpu.VMEM((rows, width), jnp.int32),
            pltpu.VMEM((rows, rows), jnp.float32),
            pltpu.VMEM((8, width), jnp.float32),
            pltpu.VMEM((n, 8, width), jnp.float32),
            pltpu.VMEM((8, width), jnp.float32),
            pltpu.VMEM((n_dp, 8, width), jnp.float32),
            dma((4,)),
            dma((2, hops, CHUNKS)),
            dma((2, hops, CHUNKS)),
            dma((2, hops, CHUNKS)),
            dma((2, hops, CHUNKS)),
            dma((n,)),
            dma((n,)),
            dma((n_dp,)),
            dma((n_dp,)),
        ],
        compiler_params=pltpu.CompilerParams(
            collective_id=0, has_side_effects=True, vmem_limit_bytes=60 * 1024 * 1024
        ),
        name="attend",
    )(doc_lengths, queries[0], keys[0], values[0], tab)
    return out[None], z[0, 0]


def solution(mesh):
    placed = (
        P("dp", "seq", None, None),
        P("dp", "seq", None, None),
        P("dp", "seq", None, None),
        P("dp", None),
    )
    return jax.shard_map(
        shards,
        mesh=mesh,
        in_specs=placed,
        out_specs=(P("dp", "seq", None, None), P()),
        check_vma=False,
    )
```

```python
import functools
import math

import jax
import jax.numpy as jnp
import numpy as np
from jax import lax
from jax.experimental import pallas as pl
from jax.experimental.pallas import tpu as pltpu
from jax.sharding import PartitionSpec as P

WINDOW = 1024
rope_base = 500000.0
score_scale = 1.0 / 12.0
masked = -1e30
MESH = pl.DeviceIdType.MESH
CHUNKS = 4
UNROLL = 8


def tables(rows, reach, width):
    half = width // 2
    frequency = rope_base ** (-2.0 * np.arange(half) / width)
    at = np.arange(rows)[None, :] - rows * np.arange(reach + 1)[:, None]
    angles = at[..., None] * frequency
    cos = np.concatenate([np.cos(angles)] * 2, axis=-1)
    sin = np.concatenate([-np.sin(angles), np.sin(angles)], axis=-1)
    return np.stack([cos, sin], axis=1).astype(np.float32)


def body(
    n, n_dp, reach, lengths, q_hbm, k_hbm, v_hbm, tab_hbm, out, z_out,
    tab, q_raw, raw, stage, spread, q_rot, weights, peaks, totals, acc, low, bias, mine, parts_seq, mine2, parts_dp,
    load_sem, z_send, z_recv, d_send, d_recv, s_send, s_recv, p_send, p_recv,
):
    rows, heads, width = k_hbm.shape
    q_heads = q_hbm.shape[1]
    group = q_heads // heads
    hops = reach // 2
    piece = rows // CHUNKS
    me = lax.axis_index("seq")
    dp = lax.axis_index("dp")
    core = lax.rem(me, 2)
    chip = me // 2
    other = me + 1 - 2 * core
    above = me + 2
    has_above = above < n
    first = core == 0
    second = core == 1

    loads = [
        pltpu.make_async_copy(k_hbm, raw.at[0, 0], load_sem.at[0]),
        pltpu.make_async_copy(v_hbm, raw.at[1, 0], load_sem.at[1]),
        pltpu.make_async_copy(q_hbm, q_raw, load_sem.at[2]),
        pltpu.make_async_copy(tab_hbm, tab, load_sem.at[3]),
    ]
    for load in loads:
        load.start()

    barrier = pltpu.get_barrier_semaphore()

    def greet_seq(j, _):
        pl.semaphore_signal(barrier, inc=1, device_id={"seq": lax.rem(me + j, n)}, device_id_type=MESH)
        return 0

    def greet_dp(j, _):
        pl.semaphore_signal(barrier, inc=1, device_id={"dp": lax.rem(dp + j, n_dp)}, device_id_type=MESH)
        return 0

    lax.fori_loop(1, n, greet_seq, 0)
    lax.fori_loop(1, n_dp, greet_dp, 0)

    peaks[...] = jnp.full_like(peaks, masked)
    totals[...] = jnp.zeros_like(totals)
    row_at = me * rows + lax.broadcasted_iota(jnp.int32, (rows, width), 0)
    start = jnp.zeros((rows, width), jnp.int32)
    end = jnp.int32(0)
    for i in range(lengths.shape[1]):
        end = end + lengths[0, i]
        start = jnp.where(end <= row_at, end, start)
    low[...] = jnp.maximum(start, row_at - (WINDOW - 1)) - me * rows

    loads[0].wait()
    loads[1].wait()
    pl.semaphore_wait(barrier, (n - 1) + (n_dp - 1))

    def up(kind, hop, i):
        return pltpu.make_async_remote_copy(
            src_ref=raw.at[kind, 2 * hop, pl.ds(i * piece, piece)],
            dst_ref=raw.at[kind, 2 * hop + 2, pl.ds(i * piece, piece)],
            send_sem=z_send.at[kind, hop, i],
            recv_sem=z_recv.at[kind, hop, i],
            device_id={"seq": above},
            device_id_type=MESH,
        )

    def across(kind, hop, i):
        there = 2 * hop + 1 - 2 * core
        slot = hop - core
        return pltpu.make_async_remote_copy(
            src_ref=raw.at[kind, 2 * hop, pl.ds(i * piece, piece)],
            dst_ref=raw.at[kind, there, pl.ds(i * piece, piece)],
            send_sem=d_send.at[kind, slot, i],
            recv_sem=d_recv.at[kind, slot, i],
            device_id={"seq": other},
            device_id_type=MESH,
        )

    def each(low_i, high_i, do):
        def step(i, _):
            do(i)
            return 0

        lax.fori_loop(low_i, high_i, step, 0)

    def send_up(kind, hop, a, b):
        @pl.when(has_above)
        def _():
            each(a, b, lambda i: up(kind, hop, i).start())

    send_up(0, 0, 0, CHUNKS)
    send_up(1, 0, 0, 1)

    @pl.when(first)
    def _():
        for kind in range(2):
            each(0, CHUNKS, lambda i: across(kind, 0, i).start())

    def take(kind, hop, a, b):
        def one(i):
            up(kind, hop - 1, i).wait_recv()
            if hop < hops:
                @pl.when(has_above)
                def _():
                    up(kind, hop, i).start()

                across(kind, hop, i).start()
            else:
                @pl.when(second)
                def _():
                    across(kind, hop, i).start()

        each(a, b, one)

    def take_across(kind, slot, a, b):
        def one(i):
            pltpu.make_async_remote_copy(
                src_ref=raw.at[kind, 0, pl.ds(i * piece, piece)],
                dst_ref=raw.at[kind, 2 * slot + 1, pl.ds(i * piece, piece)],
                send_sem=d_send.at[kind, slot, i],
                recv_sem=d_recv.at[kind, slot, i],
                device_id={"seq": other},
                device_id_type=MESH,
            ).wait_recv()

        each(a, b, one)

    loads[2].wait()
    loads[3].wait()

    stage[...] = q_raw[...].astype(jnp.float32).reshape(rows * q_heads, width)
    scale = score_scale * math.log2(math.e)

    def turn_q(h, _):
        for g in range(group):
            x = stage[pl.ds(h * group + g, rows, stride=q_heads), :]
            turned = x * tab[0, 0] + pltpu.roll(x, width // 2, 1) * tab[0, 1]
            q_rot[h, g * rows : (g + 1) * rows, :] = (turned * scale).astype(jnp.bfloat16)
        return 0

    lax.fori_loop(0, heads, turn_q, 0)

    lane = lax.broadcasted_iota(jnp.int32, (rows, width), 1)

    def score(d):
        stage[0 : rows * heads, :] = raw[0, d].astype(jnp.float32).reshape(rows * heads, width)
        key_at = lax.broadcasted_iota(jnp.int32, (rows, rows), 1) - d * rows
        query_at = lax.broadcasted_iota(jnp.int32, (rows, rows), 0)
        seen = (key_at >= low[:, 0:1]) & (key_at <= query_at)
        bias[...] = jnp.where(seen, 0.0, masked)

        def head(h, _):
            x = stage[pl.ds(h, rows, stride=heads), :]
            k = (x * tab[d, 0] + pltpu.roll(x, width // 2, 1) * tab[d, 1]).astype(jnp.bfloat16)
            for g in range(group):
                part = slice(g * rows, (g + 1) * rows)
                s = lax.dot_general(
                    q_rot[h, part, :], k, (((1,), (1,)), ((), ())), preferred_element_type=jnp.float32
                )
                s = s + bias[...]
                m = jnp.max(s, axis=1, keepdims=True)
                p = jnp.exp2(s - m)
                t = jnp.sum(p, axis=1, keepdims=True)
                weights[d, h, part, :] = p.astype(jnp.bfloat16)
                peaks[h, part, :] = jnp.where(lane == d, m, peaks[h, part, :])
                totals[h, part, :] = jnp.where(lane == d, t, totals[h, part, :])
            return 0

        lax.fori_loop(0, heads, head, 0)

    def mix(blocks, a, b, fresh=False, last=False):
        count = b - a
        for j, d in enumerate(blocks):
            stage[j * count * heads : (j + 1) * count * heads, :] = (
                raw[1, d, a:b].astype(jnp.float32).reshape(count * heads, width)
            )

        def head(h):
            v = [
                stage[pl.ds(j * count * heads + h, count, stride=heads), :].astype(jnp.bfloat16)
                for j in range(len(blocks))
            ]
            w = [weights[d, h, :, a:b] for d in blocks]
            o = jnp.dot(jnp.concatenate(w, axis=1), jnp.concatenate(v, axis=0), preferred_element_type=jnp.float32)
            if not fresh:
                o = acc[h] + o
            if last:
                for g in range(group):
                    spread[pl.ds(h * group + g, rows, stride=q_heads), :] = o[g * rows : (g + 1) * rows]
            else:
                acc[h] = o

        def pair(i, _):
            for j in range(UNROLL):
                head(i * UNROLL + j)
            return 0

        lax.fori_loop(0, heads // UNROLL, pair, 0)

    score(0)

    @pl.when(second)
    def _():
        take_across(0, 0, 0, CHUNKS)
        score(1)

    @pl.when(chip >= 1)
    def _():
        take(0, 1, 0, CHUNKS)

    send_up(1, 0, 1, CHUNKS)

    @pl.when(chip >= 1)
    def _():
        score(2)
        take_across(0, core, 0, CHUNKS)
        score(1 + 2 * core)
        take(1, 1, 0, 1)

    @pl.when(chip >= 2)
    def _():
        take(0, 2, 0, CHUNKS)
        score(4)

        @pl.when(first)
        def _():
            take_across(0, 1, 0, CHUNKS)
            score(3)

    def settle(h, square):
        m = peaks[h]
        peak = jnp.max(m, axis=1, keepdims=True)
        a = jnp.exp2(m - peak)
        total = jnp.sum(a * totals[h], axis=1, keepdims=True)
        peaks[h] = a / total
        lse = peak * math.log(2.0) + jnp.log(total)
        return square + jnp.sum(lse * lse, axis=0, keepdims=True)

    square = lax.fori_loop(0, heads, settle, jnp.zeros((1, 1), jnp.float32))
    mine[...] = jnp.broadcast_to(square, mine.shape)
    parts_seq[me] = jnp.broadcast_to(square, mine.shape)

    def tell_seq(j):
        return pltpu.make_async_remote_copy(
            src_ref=mine, dst_ref=parts_seq.at[me], send_sem=s_send.at[j], recv_sem=s_recv.at[j],
            device_id={"seq": lax.rem(me + j, n)}, device_id_type=MESH,
        )

    def heard_seq(j):
        return pltpu.make_async_remote_copy(
            src_ref=mine, dst_ref=parts_seq.at[lax.rem(me + n - j, n)], send_sem=s_send.at[j], recv_sem=s_recv.at[j],
            device_id={"seq": lax.rem(me + j, n)}, device_id_type=MESH,
        )

    def tell_dp(j):
        return pltpu.make_async_remote_copy(
            src_ref=mine2, dst_ref=parts_dp.at[dp], send_sem=p_send.at[j], recv_sem=p_recv.at[j],
            device_id={"dp": lax.rem(dp + j, n_dp)}, device_id_type=MESH,
        )

    def heard_dp(j):
        return pltpu.make_async_remote_copy(
            src_ref=mine2, dst_ref=parts_dp.at[lax.rem(dp + n_dp - j, n_dp)], send_sem=p_send.at[j], recv_sem=p_recv.at[j],
            device_id={"dp": lax.rem(dp + j, n_dp)}, device_id_type=MESH,
        )

    @pl.when(chip >= 1)
    def _():
        take(1, 1, 1, 2)

    each(1, n, lambda j: tell_seq(j).start())

    def portion(h, _):
        for d in range(reach + 1):
            weights[d, h] = (weights[d, h].astype(jnp.float32) * peaks[h, :, d : d + 1]).astype(jnp.bfloat16)
        return 0

    lax.fori_loop(0, heads, portion, 0)

    @pl.when(chip >= 1)
    def _():
        take(1, 1, 2, CHUNKS)

    @pl.when(first)
    def _():
        mix((0,), 0, rows, fresh=True)

    @pl.when(second)
    def _():
        take_across(1, 0, 0, CHUNKS)
        mix((0, 1), 0, rows, fresh=True)

    @pl.when(chip >= 1)
    def _():
        take_across(1, core, 0, CHUNKS)
        mix((2, 1 + 2 * core), 0, rows)

    each(1, n, lambda j: heard_seq(j).wait_recv())
    column = jnp.sum(parts_seq[...], axis=0)
    mine2[...] = column
    parts_dp[dp] = column

    middle = rows // 2

    @pl.when(chip >= 2)
    def _():
        take(1, 2, 0, CHUNKS // 2)

        @pl.when(second)
        def _():
            mix((4,), 0, middle)

        @pl.when(first)
        def _():
            take_across(1, 1, 0, CHUNKS // 2)
            mix((4, 3), 0, middle)

    each(1, n_dp, lambda j: tell_dp(j).start())

    @pl.when(chip >= 2)
    def _():
        take(1, 2, CHUNKS // 2, CHUNKS)

        @pl.when(second)
        def _():
            mix((4,), middle, rows, last=True)

        @pl.when(first)
        def _():
            take_across(1, 1, CHUNKS // 2, CHUNKS)
            mix((4, 3), middle, rows, last=True)

    def give(h, _):
        for g in range(group):
            spread[pl.ds(h * group + g, rows, stride=q_heads), :] = acc[h, g * rows : (g + 1) * rows, :]
        return 0

    @pl.when(chip < 2)
    def _():
        lax.fori_loop(0, heads, give, 0)

    out[...] = spread[...].reshape(rows, q_heads, width).astype(jnp.bfloat16)

    each(1, n_dp, lambda j: heard_dp(j).wait_recv())
    z_out[0, 0] = jnp.sum(jnp.sum(parts_dp[...], axis=0)[0:1, 0:1]) / (n_dp * n * rows * q_heads)

    def sent_up(kind, hop):
        each(0, CHUNKS, lambda i: up(kind, hop, i).wait_send())

    def sent_across(kind, hop):
        each(0, CHUNKS, lambda i: across(kind, hop, i).wait_send())

    for kind in range(2):
        pl.when(has_above)(functools.partial(sent_up, kind, 0))
        pl.when(has_above & (chip >= 1))(functools.partial(sent_up, kind, 1))
        pl.when(first)(functools.partial(sent_across, kind, 0))
        pl.when(chip >= 1)(functools.partial(sent_across, kind, 1))
        pl.when(second & (chip >= 2))(functools.partial(sent_across, kind, 2))
    each(1, n, lambda j: tell_seq(j).wait_send())
    each(1, n_dp, lambda j: tell_dp(j).wait_send())


def shards(queries, keys, values, doc_lengths):
    _, rows, q_heads, width = queries.shape
    heads = keys.shape[2]
    group = q_heads // heads
    n = lax.axis_size("seq")
    n_dp = lax.axis_size("dp")
    reach = -(-(WINDOW - 1) // rows)
    assert n % 2 == 0 and reach == 4
    hops = reach // 2
    tab = jnp.asarray(tables(rows, reach, width))
    vmem = pl.BlockSpec(memory_space=pltpu.VMEM)
    smem = pl.BlockSpec(memory_space=pltpu.SMEM)
    anywhere = pl.BlockSpec(memory_space=pl.ANY)
    dma = pltpu.SemaphoreType.DMA
    out, z = pl.pallas_call(
        functools.partial(body, n, n_dp, reach),
        out_shape=(
            jax.ShapeDtypeStruct((rows, q_heads, width), jnp.bfloat16),
            jax.ShapeDtypeStruct((1, 1), jnp.float32),
        ),
        in_specs=[smem, anywhere, anywhere, anywhere, anywhere],
        out_specs=(vmem, smem),
        scratch_shapes=[
            pltpu.VMEM(tab.shape, jnp.float32),
            pltpu.VMEM((rows, q_heads, width), jnp.bfloat16),
            pltpu.VMEM((2, reach + 1, rows, heads, width), jnp.bfloat16),
            pltpu.VMEM((rows * q_heads, width), jnp.float32),
            pltpu.VMEM((rows * q_heads, width), jnp.float32),
            pltpu.VMEM((heads, group * rows, width), jnp.bfloat16),
            pltpu.VMEM((reach + 1, heads, group * rows, rows), jnp.bfloat16),
            pltpu.VMEM((heads, group * rows, width), jnp.float32),
            pltpu.VMEM((heads, group * rows, width), jnp.float32),
            pltpu.VMEM((heads, group * rows, width), jnp.float32),
            pltpu.VMEM((rows, width), jnp.int32),
            pltpu.VMEM((rows, rows), jnp.float32),
            pltpu.VMEM((8, width), jnp.float32),
            pltpu.VMEM((n, 8, width), jnp.float32),
            pltpu.VMEM((8, width), jnp.float32),
            pltpu.VMEM((n_dp, 8, width), jnp.float32),
            dma((4,)),
            dma((2, hops, CHUNKS)),
            dma((2, hops, CHUNKS)),
            dma((2, hops, CHUNKS)),
            dma((2, hops, CHUNKS)),
            dma((n,)),
            dma((n,)),
            dma((n_dp,)),
            dma((n_dp,)),
        ],
        compiler_params=pltpu.CompilerParams(
            collective_id=0, has_side_effects=True, vmem_limit_bytes=60 * 1024 * 1024
        ),
        name="attend",
    )(doc_lengths, queries[0], keys[0], values[0], tab)
    return out[None], z[0, 0]


def solution(mesh):
    placed = (
        P("dp", "seq", None, None),
        P("dp", "seq", None, None),
        P("dp", "seq", None, None),
        P("dp", None),
    )
    return jax.shard_map(
        shards,
        mesh=mesh,
        in_specs=placed,
        out_specs=(P("dp", "seq", None, None), P()),
        check_vma=False,
    )
```
